1024 devices in a mesh: row: 16 (over z_hi, x), col: 64 (over z_lo, y, core).
Axes of the slice: x: 4, y: 8, z: 16 (z_hi: 4, z_lo: 4; z = z_hi * 4 + z_lo), core: 2. Of those that a mesh axis runs over, the one named last changes fastest.
Arguments:
- queries: bfloat16 [64, 2048, 1024], P('col', 'row'), may hold values from -120 to 120
- keys: bfloat16 [64, 2048, 128], P('col', 'row'), may hold values from -8 to 8
- values: bfloat16 [64, 2048, 128], P('col', 'row'), may hold values from -6 to 6
- outputs: bfloat16 [64, 2048, 1024], P('col', 'row'), may hold values from -6 to 6
- out_grad: bfloat16 [64, 2048, 1024], P('col', 'row'), may hold values from -192 to 192
- positions: int32 [64, 2048], P('col'), may hold values from 0 to 2047, each once within a row
- tile_flags: int32 [64, 16, 16], P('col', 'row'), may hold values 0 or 1
Outputs:
- query_grad: bfloat16 [64, 2048, 1024], P('col', 'row')
- key_grad: bfloat16 [64, 2048, 128], P('col', 'row')
- value_grad: bfloat16 [64, 2048, 128], P('col', 'row')
The draws below stay inside these ranges and needn't reach their ends.
All inputs are finite; a program needn't handle non-finite values. No bound on the sum of `tile_flags` on one device may be relied on, other than what follows from the above.
Results may differ from the reference program's by a relative error of at most 0.0065.
Values may be sent and summed in bfloat16 or wider, within the bound.
A program may use at most 64 MiB of HBM per device.

```python
import math
import jax
import jax.numpy as jnp
from jax import lax

H = 8
HD = 128
TOK_DEV = 128
LENGTH = 2048
SEQS = 64
N_ROW = 16


def shared_draw(key):
    base_key = jax.random.fold_in(key, 7)
    first_key, second_key = jax.random.split(base_key, 2)
    total = SEQS * LENGTH
    key_rows = jnp.clip(jax.random.normal(first_key, (total, HD), jnp.float32), -6.0, 6.0)
    query_rows = jnp.clip(jax.random.normal(second_key, (total, H, HD), jnp.float32), -6.0, 6.0)
    return (query_rows.reshape(SEQS, LENGTH, H * HD), key_rows.reshape(SEQS, LENGTH, HD))


def draw_queries(key, part):
    return shared_draw(key)[0].astype(jnp.bfloat16)


def draw_keys(key, part):
    return shared_draw(key)[1].astype(jnp.bfloat16)


def set_ends(result, own_key, least, largest):
    dims = result.shape
    place = [jax.random.randint(jax.random.fold_in(own_key, axis), (), 0, dims[axis]) for axis in range(len(dims))]
    result = result.at[tuple(place)].set(least)
    longest = dims.index(max(dims))
    place[longest] = (place[longest] + 1) % dims[longest]
    return result.at[tuple(place)].set(largest)


def levels(stream_key, dims, cuts, least, largest):
    def one(dim, blocks):
        draws = jax.random.uniform(jax.random.fold_in(jax.random.fold_in(stream_key, 6), dim), (blocks,), jnp.float32, least / len(cuts), largest / len(cuts))
        return jnp.repeat(jnp.exp(draws), dims[dim] // blocks).reshape((-1,) + (1,) * (len(dims) - dim - 1))

    level = one(*cuts[0])
    for cut in cuts[1:]:
        level = level * one(*cut)
    return level


def normal_values(own_key, extent, scale, bound, cuts=(), kind=jnp.bfloat16):
    drawn = scale * jax.random.normal(own_key, extent, jnp.float32)
    if cuts:
        drawn = drawn * levels(own_key, extent, cuts, -0.22, 0.18)
    return jnp.clip(drawn, -bound, bound).astype(kind)


def setup_inputs(seed: int = 0) -> dict:
    streams_of = jax.random.split(jax.random.key(seed), 8)
    queries = draw_queries(jax.random.fold_in(streams_of[7], 71), 0)
    keys = draw_keys(jax.random.fold_in(streams_of[7], 71), 0)
    values = normal_values(streams_of[2], (SEQS, LENGTH, HD), 1.0, 6.0, ((0, 64), (1, 16)))
    outputs = normal_values(streams_of[3], (SEQS, LENGTH, H * HD), 1.0, 6.0, ((0, 64), (1, 16)))
    out_grad = normal_values(streams_of[4], (SEQS, LENGTH, H * HD), 32.0, 192.0, ((0, 64), (1, 16)))
    positions = jax.vmap(lambda own: jax.random.permutation(own, LENGTH))(jax.random.split(streams_of[5], SEQS)).reshape((SEQS, LENGTH)).astype(jnp.int32)
    tile_flags = set_ends((jax.random.randint(streams_of[6], (SEQS, N_ROW, N_ROW), 0, 2) < 1).astype(jnp.int32), jax.random.fold_in(streams_of[6], 1), 0, 1)
    return dict(queries=queries, keys=keys, values=values, outputs=outputs, out_grad=out_grad, positions=positions, tile_flags=tile_flags)


def one_trace(trace_in):
    query_seq, key_seq, value_seq, output_seq, grad_seq, pos_seq, flag_seq = trace_in
    score_scale = 1.0 / math.sqrt(HD)
    key_rows = key_seq.astype(jnp.float32)
    value_rows = value_seq.astype(jnp.float32)
    key_index = jnp.arange(LENGTH, dtype=jnp.int32)
    key_group = key_index // TOK_DEV

    def per_block(totals, block_in):
        key_total, value_total = totals
        query_block, grad_block, output_block, block_at = block_in
        query_heads = query_block.reshape(TOK_DEV, H, HD).astype(jnp.float32)
        grad_heads = grad_block.reshape(TOK_DEV, H, HD).astype(jnp.float32)
        output_heads = output_block.reshape(TOK_DEV, H, HD).astype(jnp.float32)
        query_index = block_at * TOK_DEV + jnp.arange(TOK_DEV, dtype=jnp.int32)
        query_pos = lax.dynamic_slice_in_dim(pos_seq, (block_at * TOK_DEV).astype(jnp.int32), TOK_DEV)
        key_flags = flag_seq[block_at][key_group]
        allowed = (pos_seq[None, :] <= query_pos[:, None]) & ((key_flags[None, :] == 1) | (key_index[None, :] == query_index[:, None]))
        scores = jnp.einsum('qhd,kd->hqk', query_heads, key_rows) * score_scale
        masked = jnp.where(allowed[None], scores, -1e+30)
        row_max = lax.optimization_barrier(jnp.max(masked, axis=2, keepdims=True))
        row_sum = lax.optimization_barrier(jnp.sum(jnp.where(allowed[None], jnp.exp(masked - row_max), 0.0), axis=2, keepdims=True))
        log_total = row_max + jnp.log(row_sum)
        weights = jnp.where(allowed[None], jnp.exp(masked - log_total), 0.0)
        out_dot = lax.optimization_barrier(jnp.sum(grad_heads * output_heads, axis=2)).T
        grad_probs = jnp.einsum('qhd,kd->hqk', grad_heads, value_rows)
        grad_scores = (weights * (grad_probs - out_dot[:, :, None]) * score_scale).astype(jnp.bfloat16)
        weights_low = weights.astype(jnp.bfloat16)
        grad_query = jnp.einsum('hqk,kd->qhd', grad_scores.astype(jnp.float32), key_rows)
        grad_query = grad_query.reshape(TOK_DEV, H * HD).astype(jnp.bfloat16)
        key_total = key_total + jnp.einsum('hqk,qhd->kd', grad_scores.astype(jnp.float32), query_heads)
        value_total = value_total + jnp.einsum('hqk,qhd->kd', weights_low.astype(jnp.float32), grad_heads)
        return ((key_total, value_total), grad_query)
    zeros = jnp.zeros((LENGTH, HD), jnp.float32)
    block_ids = jnp.arange(N_ROW, dtype=jnp.int32)
    block_in = (query_seq.reshape(N_ROW, TOK_DEV, H * HD), grad_seq.reshape(N_ROW, TOK_DEV, H * HD), output_seq.reshape(N_ROW, TOK_DEV, H * HD), block_ids)
    (key_total, value_total), query_grad = lax.scan(per_block, (zeros, zeros), block_in)
    return (query_grad.reshape(LENGTH, H * HD), key_total.astype(jnp.bfloat16), value_total.astype(jnp.bfloat16))

def reference(queries, keys, values, outputs, out_grad, positions, tile_flags):
    return lax.map(one_trace, (queries, keys, values, outputs, out_grad, positions, tile_flags))
```

```python
import functools
import math

import jax
import jax.numpy as jnp
from jax import lax
from jax.experimental import pallas as pl
from jax.experimental.pallas import tpu as pltpu
from jax.sharding import PartitionSpec as P

H = 8
HD = 128
T = 128
R = 4
HT = H * T
CH = 256
NEG = -1e30
SCALE = 1.0 / math.sqrt(HD)
LOG2E = math.log2(math.e)
NT = (((1,), (1,)), ((), ()))
F32 = jnp.float32
BF16 = jnp.bfloat16
GROUPS = (2, 1, 3, 0)


def kernel(
    q_hbm, k_hbm, v_hbm, o_hbm, g_hbm, pos_ref, flag_ref,
    dq_hbm, dk_ref, dv_ref,
    q_in, o_in, g_in, qs, gs, kv, kt, pos_rows, bias, sbuf, dsbuf,
    top, total, lse, dot_row, pf, tx, xrl, xin, xsum, ztx, zrl, zin, dq_out,
    in_sem, out_sem, gather_send, gather_recv, sum_send, sum_recv,
):
    me = lax.axis_index("row")
    zh = me // R
    x = me % R
    z_dev = {1: ((zh + 1) % R) * R + x, -1: ((zh + R - 1) % R) * R + x}
    x_dev = {1: zh * R + (x + 1) % R, -1: zh * R + (x + R - 1) % R}

    k_copy = pltpu.make_async_copy(k_hbm.at[0], kv.at[0, 0, 0], in_sem.at[0])
    v_copy = pltpu.make_async_copy(v_hbm.at[0], kv.at[0, 0, 1], in_sem.at[1])
    g_copy = pltpu.make_async_copy(g_hbm.at[0], g_in, in_sem.at[2])
    o_copy = pltpu.make_async_copy(o_hbm.at[0], o_in, in_sem.at[3])
    q_copy = pltpu.make_async_copy(q_hbm.at[0], q_in, in_sem.at[4])
    for copy in (k_copy, v_copy, q_copy, g_copy, o_copy):
        copy.start()

    barrier = pltpu.get_barrier_semaphore()
    for dev in (x_dev[1], x_dev[-1], z_dev[1], z_dev[-1]):
        pl.semaphore_signal(
            barrier, inc=1, device_id={"row": dev}, device_id_type=pl.DeviceIdType.MESH
        )

    sent = []

    def remote(src, dst, send, recv, dev):
        copy = pltpu.make_async_remote_copy(
            src_ref=src, dst_ref=dst, send_sem=send, recv_sem=recv,
            device_id={"row": dev}, device_id_type=pl.DeviceIdType.MESH,
        )
        copy.start()
        sent.append(copy)
        return copy

    incoming = {}

    def give(rz, rx, kind, to_rz, to_rx, dev):
        incoming[to_rz, to_rx, kind] = remote(
            kv.at[rz, rx, kind], kv.at[to_rz, to_rx, kind],
            gather_send.at[to_rz, to_rx, kind], gather_recv.at[to_rz, to_rx, kind], dev,
        )

    def got(*slot):
        incoming[slot].wait_recv()

    def along_x(rz):
        give(rz, 0, 0, rz, 3, x_dev[1])
        give(rz, 0, 1, rz, 1, x_dev[-1])
        give(rz, 0, 1, rz, 3, x_dev[1])
        give(rz, 0, 0, rz, 1, x_dev[-1])

    def onward_x(rz):
        got(rz, 3, 0)
        give(rz, 3, 0, rz, 2, x_dev[1])
        got(rz, 1, 1)
        give(rz, 1, 1, rz, 2, x_dev[-1])

    def rest_x(rz):
        got(rz, 3, 1)
        got(rz, 1, 0)
        got(rz, 2, 0)
        got(rz, 2, 1)

    pos_rows[...] = jnp.zeros_like(pos_rows)
    for slot in range(R * R):
        block = ((zh + slot // R) % R) * R + (x + slot % R) % R
        row = pos_ref[:, pl.ds(pl.multiple_of(block * T, T), T)]
        pos_rows[slot : slot + 1, :] = row.astype(F32)

    k_copy.wait()
    v_copy.wait()
    pl.semaphore_wait(barrier, 4)

    give(0, 0, 0, 3, 0, z_dev[1])
    give(0, 0, 1, 1, 0, z_dev[-1])
    give(0, 0, 1, 3, 0, z_dev[1])
    give(0, 0, 0, 1, 0, z_dev[-1])
    along_x(0)

    pos_cols = pos_rows[...].T
    own_pos = pos_rows[0:1, :]
    for slot in range(R * R):
        block = ((zh + slot // R) % R) * R + (x + slot % R) % R
        off = (flag_ref[0, 0, block] - 1).astype(F32) * (-NEG)
        column = jnp.broadcast_to(pos_cols[:, slot : slot + 1], (T, T))
        value = jnp.where(column <= own_pos, 0.0, NEG) + off
        if slot == 0:
            keys_at = lax.broadcasted_iota(jnp.int32, (T, T), 0)
            queries_at = lax.broadcasted_iota(jnp.int32, (T, T), 1)
            value = jnp.where(keys_at == queries_at, 0.0, value)
        bias[slot] = value

    q_copy.wait()
    for h in range(H):
        qs[h * T : (h + 1) * T, :] = q_in[:, h * HD : (h + 1) * HD]
    g_copy.wait()
    o_copy.wait()
    for h in range(H):
        cols = slice(h * HD, (h + 1) * HD)
        gs[h * T : (h + 1) * T, :] = g_in[:, cols]
        product = g_in[:, cols].astype(F32) * o_in[:, cols].astype(F32)
        dot_row[:, h * T : (h + 1) * T] = jnp.sum(product.T, axis=0, keepdims=True)

    top[...] = jnp.full_like(top, NEG)
    total[...] = jnp.zeros_like(total)

    def score_block(rz, rx):
        slot = rz * R + rx
        key_block = kv[rz, rx, 0]
        kt[slot] = key_block.T
        mask = bias[slot]
        mask = jnp.concatenate([mask] * (CH // T), axis=1)
        for c in range(HT // CH):
            part = slice(c * CH, (c + 1) * CH)
            raw = lax.dot_general(key_block, qs[part, :], NT, preferred_element_type=F32)
            score = raw * (SCALE * LOG2E) + mask
            sbuf[slot, :, part] = score
            parts = score.reshape(T // 8, 8, CH)
            old = top[:, part]
            new = jnp.maximum(old, jnp.max(parts, axis=0))
            added = jnp.sum(jnp.exp2(parts - new[None]), axis=0)
            total[:, part] = total[:, part] * jnp.exp2(old - new) + added
            top[:, part] = new

    def score_group(rz):
        def step(rx, carry):
            score_block(rz, rx)
            return carry

        lax.fori_loop(0, R, step, 0)

    onward_x(0)
    got(3, 0, 0)
    give(3, 0, 0, 2, 0, z_dev[1])
    got(1, 0, 1)
    give(1, 0, 1, 2, 0, z_dev[-1])
    got(3, 0, 1)
    along_x(3)
    got(1, 0, 0)
    along_x(1)
    rest_x(0)
    score_group(0)
    onward_x(3)
    onward_x(1)
    got(2, 0, 0)
    got(2, 0, 1)
    along_x(2)
    rest_x(3)
    score_group(3)
    rest_x(1)
    score_group(1)
    onward_x(2)
    rest_x(2)
    score_group(2)

    top_all = jnp.max(top[...], axis=0, keepdims=True)
    total_all = jnp.sum(total[...] * jnp.exp2(top[...] - top_all), axis=0, keepdims=True)
    lse[...] = top_all + jnp.log(total_all) * LOG2E

    def grad_block(rz, rx):
        slot = rz * R + rx
        value_block = kv[rz, rx, 1]
        dk = jnp.zeros((T, HD), F32)
        dv = jnp.zeros((T, HD), F32)
        for c in range(HT // CH):
            part = slice(c * CH, (c + 1) * CH)
            weights = jnp.exp2(sbuf[slot, :, part] - lse[:, part])
            probs = lax.dot_general(value_block, gs[part, :], NT, preferred_element_type=F32)
            grads = (weights * (probs - dot_row[:, part]) * SCALE).astype(BF16)
            dsbuf[slot, :, part] = grads
            dk = dk + jnp.dot(grads, qs[part, :], preferred_element_type=F32)
            dv = dv + jnp.dot(weights.astype(BF16), gs[part, :], preferred_element_type=F32)
        pf[rz, rx, 0] = dk
        pf[rz, rx, 1] = dv
        tx[rz, rx, 0] = dk.astype(BF16)
        tx[rz, rx, 1] = dv.astype(BF16)

    def grad_group(rz):
        def step(rx, carry):
            grad_block(rz, rx)
            return carry

        lax.fori_loop(0, R, step, 0)

    sums = {}

    def give_sum(group, what, src, dst, dev):
        sums[group, what] = remote(
            src, dst, sum_send.at[group, what], sum_recv.at[group, what], dev
        )

    def x_first(rz):
        give_sum(rz, 0, tx.at[rz, 2, 0], xrl.at[rz, 0], x_dev[1])
        give_sum(rz, 1, tx.at[rz, 2, 1], xrl.at[rz, 1], x_dev[-1])
        give_sum(rz, 2, tx.at[rz, 1, 1], xin.at[rz, 0, 1], x_dev[1])
        give_sum(rz, 3, tx.at[rz, 3, 0], xin.at[rz, 1, 0], x_dev[-1])

    def x_second(rz):
        sums[rz, 0].wait_recv()
        tx[rz, 1, 0] = (pf[rz, 1, 0] + xrl[rz, 0].astype(F32)).astype(BF16)
        give_sum(rz, 4, tx.at[rz, 1, 0], xin.at[rz, 0, 0], x_dev[1])
        sums[rz, 1].wait_recv()
        tx[rz, 3, 1] = (pf[rz, 3, 1] + xrl[rz, 1].astype(F32)).astype(BF16)
        give_sum(rz, 5, tx.at[rz, 3, 1], xin.at[rz, 1, 1], x_dev[-1])

    def x_sum(rz):
        for what in (2, 3, 4, 5):
            sums[rz, what].wait_recv()
        for kind in range(2):
            both = xin[rz, 0, kind].astype(F32) + xin[rz, 1, kind].astype(F32)
            xsum[rz, kind] = pf[rz, 0, kind] + both

    def to_z(rz, kind):
        ztx[rz, kind] = xsum[rz, kind].astype(BF16)

    grad_group(2)
    x_first(2)
    grad_group(1)
    x_first(1)
    x_second(2)
    grad_group(3)
    x_first(3)
    x_second(1)
    x_sum(2)
    to_z(2, 0)
    give_sum(R, 0, ztx.at[2, 0], zrl.at[0], z_dev[1])
    to_z(2, 1)
    give_sum(R, 1, ztx.at[2, 1], zrl.at[1], z_dev[-1])
    grad_group(0)
    x_first(0)
    x_second(3)
    x_sum(1)
    to_z(1, 1)
    give_sum(R, 2, ztx.at[1, 1], zin.at[0, 1], z_dev[1])
    x_second(0)
    x_sum(3)
    to_z(3, 0)
    give_sum(R, 3, ztx.at[3, 0], zin.at[1, 0], z_dev[-1])

    for c in range(HT // CH):
        grad_t = jnp.zeros((HD, CH), F32)
        for slot in range(0, R * R):
            grad_t = grad_t + jnp.dot(
                kt[slot], dsbuf[slot, :, c * CH : (c + 1) * CH], preferred_element_type=F32
            )
        for part in range(CH // T):
            h = c * (CH // T) + part
            head = grad_t[:, part * T : (part + 1) * T]
            dq_out[:, h * HD : (h + 1) * HD] = head.T.astype(BF16)
    dq_copy = pltpu.make_async_copy(dq_out, dq_hbm.at[0], out_sem.at[0])
    dq_copy.start()

    sums[R, 0].wait_recv()
    ztx[1, 0] = (xsum[1, 0] + zrl[0].astype(F32)).astype(BF16)
    give_sum(R, 4, ztx.at[1, 0], zin.at[0, 0], z_dev[1])
    sums[R, 1].wait_recv()
    ztx[3, 1] = (xsum[3, 1] + zrl[1].astype(F32)).astype(BF16)
    give_sum(R, 5, ztx.at[3, 1], zin.at[1, 1], z_dev[-1])
    x_sum(0)
    for what in (2, 3, 4, 5):
        sums[R, what].wait_recv()
    for kind, out in ((0, dk_ref), (1, dv_ref)):
        both = zin[0, kind].astype(F32) + zin[1, kind].astype(F32)
        out[0] = (xsum[0, kind] + both).astype(BF16)

    for copy in sent:
        copy.wait_send()
    dq_copy.wait()


def body(queries, keys, values, outputs, out_grad, positions, tile_flags):
    block = jax.ShapeDtypeStruct((1, T, HD), BF16)
    hbm = pl.BlockSpec(memory_space=pl.ANY)
    vmem = pl.BlockSpec(memory_space=pltpu.VMEM)
    dma = pltpu.SemaphoreType.DMA
    return pl.pallas_call(
        kernel,
        out_shape=(jax.ShapeDtypeStruct((1, T, H * HD), BF16), block, block),
        in_specs=[hbm] * 5 + [vmem, pl.BlockSpec(memory_space=pltpu.SMEM)],
        out_specs=(hbm, vmem, vmem),
        scratch_shapes=[
            pltpu.VMEM((T, H * HD), BF16),
            pltpu.VMEM((T, H * HD), BF16),
            pltpu.VMEM((T, H * HD), BF16),
            pltpu.VMEM((HT, HD), BF16),
            pltpu.VMEM((HT, HD), BF16),
            pltpu.VMEM((R, R, 2, T, HD), BF16),
            pltpu.VMEM((R * R, HD, T), BF16),
            pltpu.VMEM((T, T), F32),
            pltpu.VMEM((R * R, T, T), F32),
            pltpu.VMEM((R * R, T, HT), F32),
            pltpu.VMEM((R * R, T, HT), BF16),
            pltpu.VMEM((8, HT), F32),
            pltpu.VMEM((8, HT), F32),
            pltpu.VMEM((1, HT), F32),
            pltpu.VMEM((1, HT), F32),
            pltpu.VMEM((R, R, 2, T, HD), F32),
            pltpu.VMEM((R, R, 2, T, HD), BF16),
            pltpu.VMEM((R, 2, T, HD), BF16),
            pltpu.VMEM((R, 2, 2, T, HD), BF16),
            pltpu.VMEM((R, 2, T, HD), F32),
            pltpu.VMEM((R, 2, T, HD), BF16),
            pltpu.VMEM((2, T, HD), BF16),
            pltpu.VMEM((2, 2, T, HD), BF16),
            pltpu.VMEM((T, H * HD), BF16),
            dma((5,)),
            dma((1,)),
            dma((R, R, 2)),
            dma((R, R, 2)),
            dma((R + 1, 6)),
            dma((R + 1, 6)),
        ],
        compiler_params=pltpu.CompilerParams(
            collective_id=0, has_side_effects=True, vmem_limit_bytes=56 * 1024 * 1024
        ),
        name="attention_backward",
    )(queries, keys, values, outputs, out_grad, positions, tile_flags)


def solution(mesh):
    sharded = P("col", "row", None)
    placed = (sharded,) * 5 + (P("col", None), sharded)
    return jax.shard_map(
        body, mesh=mesh, in_specs=placed, out_specs=(sharded,) * 3, check_vma=False
    )
```

```python
import math

import jax
import jax.numpy as jnp
from jax import lax
from jax.experimental import pallas as pl
from jax.experimental.pallas import tpu as pltpu
from jax.sharding import PartitionSpec as P

H = 8
HD = 128
T = 128
R = 4
HT = H * T
CH = 256
NEG = -1e30
SCALE = 1.0 / math.sqrt(HD)
LOG2E = math.log2(math.e)
F32 = jnp.float32
BF16 = jnp.bfloat16
RX = (2, 1, 3, 0)
PLACE = {rx: place for place, rx in enumerate(RX)}
HALF = T // 2


def kernel(
    q_hbm, k_hbm, v_hbm, o_hbm, g_hbm, pos_hbm, flag_hbm,
    dq_hbm, dk_ref, dv_ref,
    q_in, o_in, g_in, pos_ref, flag_ref, qs, gs, q_cols, g_cols, kv, kt, pos_rows, bias, sbuf, dsbuf,
    top, total, lse, dot_row, pf, tx, xrl, xin, xsum, ztx, zrl, zin, dq_out,
    in_sem, out_sem, gather_send, gather_recv, x_send, x_recv, z_send, z_recv,
):
    me = lax.axis_index("row")
    zh = me // R
    x = me % R
    z_dev = {1: ((zh + 1) % R) * R + x, -1: ((zh + R - 1) % R) * R + x}
    x_dev = {1: zh * R + (x + 1) % R, 2: zh * R + (x + 2) % R, -1: zh * R + (x + R - 1) % R}

    own = PLACE[0]
    k_copy = pltpu.make_async_copy(k_hbm.at[0], kv.at[0, 0, own], in_sem.at[0])
    v_copy = pltpu.make_async_copy(v_hbm.at[0], kv.at[1, 0, own], in_sem.at[1])
    g_copy = pltpu.make_async_copy(g_hbm.at[0], g_in, in_sem.at[2])
    o_copy = pltpu.make_async_copy(o_hbm.at[0], o_in, in_sem.at[3])
    q_copy = pltpu.make_async_copy(q_hbm.at[0], q_in, in_sem.at[4])
    pos_copy = pltpu.make_async_copy(pos_hbm, pos_ref, in_sem.at[5])
    flag_copy = pltpu.make_async_copy(flag_hbm, flag_ref, in_sem.at[6])
    for copy in (k_copy, v_copy, pos_copy, flag_copy, q_copy, g_copy, o_copy):
        copy.start()

    barrier = pltpu.get_barrier_semaphore()
    for dev in (z_dev[1], z_dev[-1], x_dev[1], x_dev[2], x_dev[-1]):
        pl.semaphore_signal(
            barrier, inc=1, device_id={"row": dev}, device_id_type=pl.DeviceIdType.MESH
        )

    sent = []

    def remote(src, dst, send, recv, dev):
        copy = pltpu.make_async_remote_copy(
            src_ref=src, dst_ref=dst, send_sem=send, recv_sem=recv,
            device_id={"row": dev}, device_id_type=pl.DeviceIdType.MESH,
        )
        copy.start()
        sent.append(copy)
        return copy

    late = []

    def drain(copies):
        while copies:
            copies.pop().wait_send()

    incoming = {}

    def give(kind, src, dst, dev, halves=(None,)):
        (rz, rx), (to_rz, to_rx) = src, dst
        at, to = PLACE[rx], PLACE[to_rx]
        for half in halves:
            rows = pl.ds(0, T) if half is None else pl.ds(half * HALF, HALF)
            incoming.setdefault((kind, dst), []).append(
                remote(
                    kv.at[kind, rz, at, rows, :], kv.at[kind, to_rz, to, rows, :],
                    gather_send.at[kind, half or 0, to_rz, to],
                    gather_recv.at[kind, half or 0, to_rz, to], dev,
                )
            )

    def got(kind, slot):
        for copy in incoming.pop((kind, slot), ()):
            copy.wait_recv()

    def along_z():
        give(0, (0, 0), (3, 0), z_dev[1], (0, 1))
        give(1, (0, 0), (1, 0), z_dev[-1], (0, 1))
        give(1, (0, 0), (3, 0), z_dev[1])
        give(0, (0, 0), (1, 0), z_dev[-1])

    def onward_z():
        for half in range(2):
            for kind, slot, dev in ((0, (3, 0), z_dev[1]), (1, (1, 0), z_dev[-1])):
                incoming[kind, slot].pop(0).wait_recv()
                give(kind, slot, (2, 0), dev, (half,))

    def along_x(rz):
        give(0, (rz, 0), (rz, 3), x_dev[1])
        give(1, (rz, 0), (rz, 1), x_dev[-1])
        give(1, (rz, 0), (rz, 3), x_dev[1])
        give(0, (rz, 0), (rz, 1), x_dev[-1])

    def onward_x(rz, kinds=(0, 1)):
        for kind in kinds:
            slot = (rz, 1 if kind else 3)
            got(kind, slot)
            give(kind, slot, (rz, 2), x_dev[-1 if kind else 1])

    def all_of(kind, rz):
        for rx in range(R):
            got(kind, (rz, rx))

    def block_of(rz, place):
        return ((zh + rz) % R) * R + (x + RX[place]) % R

    slots = [(rz, place) for rz in range(R) for place in range(R)]
    k_copy.wait()
    v_copy.wait()
    pl.semaphore_wait(barrier, 5)

    along_z()
    along_x(0)

    pos_copy.wait()
    flag_copy.wait()
    pos_rows[...] = jnp.zeros_like(pos_rows)
    for i, slot in enumerate(slots):
        row = pos_ref[:, pl.ds(pl.multiple_of(block_of(*slot) * T, T), T)]
        pos_rows[i : i + 1, :] = row.astype(F32)
    pos_cols = pos_rows[...].T
    for i, (rz, place) in enumerate(slots):
        own_pos = pos_rows[own : own + 1, :]
        off = (flag_ref[0, 0, block_of(rz, place)] - 1).astype(F32) * (-NEG)
        column = jnp.broadcast_to(pos_cols[:, i : i + 1], (T, T))
        value = jnp.where(column <= own_pos, 0.0, NEG) + off
        if (rz, place) == (0, own):
            keys_at = lax.broadcasted_iota(jnp.int32, (T, T), 0)
            queries_at = lax.broadcasted_iota(jnp.int32, (T, T), 1)
            value = jnp.where(keys_at == queries_at, 0.0, value)
        bias[rz, place] = value

    q_copy.wait()
    for h in range(H):
        head = q_in[:, h * HD : (h + 1) * HD]
        qs[h * T : (h + 1) * T, :] = head
        q_cols[:, h * T : (h + 1) * T] = head.T
    g_copy.wait()
    o_copy.wait()
    for h in range(H):
        cols = slice(h * HD, (h + 1) * HD)
        head = g_in[:, cols]
        gs[h * T : (h + 1) * T, :] = head
        g_cols[:, h * T : (h + 1) * T] = head.T
        product = head.astype(F32) * o_in[:, cols].astype(F32)
        dot_row[:, h * T : (h + 1) * T] = jnp.sum(product.T, axis=0, keepdims=True)

    top[...] = jnp.full_like(top, NEG)
    total[...] = jnp.zeros_like(total)

    def pair_of(p):
        return pl.ds(2 * p, 2)

    def score_pair(rz, p):
        pair = pair_of(p)
        keys_2 = kv[0, rz, pair].reshape(2 * T, HD)
        kt[rz, p] = keys_2.T
        mask = bias[rz, pair].reshape(2 * T, T)
        mask = jnp.concatenate([mask] * (CH // T), axis=1)
        for c in range(HT // CH):
            part = slice(c * CH, (c + 1) * CH)
            raw = jnp.dot(keys_2, q_cols[:, part], preferred_element_type=F32)
            score = raw * (SCALE * LOG2E) + mask
            sbuf[rz, pair, :, part] = score.reshape(2, T, CH)
            parts = score.reshape(2 * T // 8, 8, CH)
            old = top[:, part]
            new = jnp.maximum(old, jnp.max(parts, axis=0))
            added = jnp.sum(jnp.exp2(parts - new[None]), axis=0)
            total[:, part] = total[:, part] * jnp.exp2(old - new) + added
            top[:, part] = new

    def score_group(rz):
        def step(p, carry):
            score_pair(rz, p)
            return carry

        lax.fori_loop(0, 2, step, 0)

    onward_x(0)
    onward_z()
    got(1, (3, 0))
    along_x(3)
    got(0, (1, 0))
    along_x(1)
    all_of(0, 0)
    score_group(0)
    onward_x(3)
    onward_x(1)
    all_of(0, 3)
    score_group(3)
    got(0, (2, 0))
    give(0, (2, 0), (2, 2), x_dev[2])
    give(0, (2, 0), (2, 3), x_dev[1])
    give(0, (2, 0), (2, 1), x_dev[-1])
    got(1, (2, 0))
    give(1, (2, 0), (2, 1), x_dev[-1])
    give(1, (2, 0), (2, 3), x_dev[1])
    all_of(0, 1)
    score_group(1)
    onward_x(2, (1,))
    got(0, (2, 3))
    score_pair(2, 1)
    all_of(0, 2)
    score_pair(2, 0)

    top_all = jnp.max(top[...], axis=0, keepdims=True)
    total_all = jnp.sum(total[...] * jnp.exp2(top[...] - top_all), axis=0, keepdims=True)
    lse[...] = top_all + jnp.log(total_all) * LOG2E
    for rz in (2, 1, 3, 0):
        all_of(1, rz)

    def grad_pair(rz, p):
        pair = pair_of(p)
        values_2 = kv[1, rz, pair].reshape(2 * T, HD)
        dk = dv = None
        for c in range(HT // CH):
            part = slice(c * CH, (c + 1) * CH)
            probs = jnp.dot(values_2, g_cols[:, part], preferred_element_type=F32)
            weights = jnp.exp2(sbuf[rz, pair, :, part].reshape(2 * T, CH) - lse[:, part])
            grads = (weights * (probs - dot_row[:, part]) * SCALE).astype(BF16)
            dsbuf[rz, pair, :, part] = grads.reshape(2, T, CH)
            dk_c = jnp.dot(grads, qs[part, :], preferred_element_type=F32)
            dv_c = jnp.dot(weights.astype(BF16), gs[part, :], preferred_element_type=F32)
            dk = dk_c if c == 0 else dk + dk_c
            dv = dv_c if c == 0 else dv + dv_c
        for kind, grad in ((0, dk), (1, dv)):
            grad = grad.reshape(2, T, HD)
            pf[kind, rz, pair] = grad
            tx[kind, rz, pair] = grad.astype(BF16)

    sums = {}

    def give_x(rz, what, src, dst, dev):
        sums[rz, what] = remote(src, dst, x_send.at[rz, what], x_recv.at[rz, what], dev)

    def x_first(rz, p):
        if rz == 2 and p == 0:
            for kind in range(2):
                give_x(rz, kind, tx.at[kind, rz, PLACE[2]], xrl.at[rz, kind], x_dev[2])
            for kind, what in ((0, 4), (1, 2)):
                give_x(rz, what, tx.at[kind, rz, PLACE[1]], xin.at[rz, 0, kind], x_dev[1])
        elif rz == 2:
            for kind, what in ((0, 3), (1, 5)):
                give_x(rz, what, tx.at[kind, rz, PLACE[3]], xin.at[rz, 1, kind], x_dev[-1])
        elif p == 0:
            give_x(rz, 0, tx.at[0, rz, PLACE[2]], xrl.at[rz, 0], x_dev[1])
            give_x(rz, 1, tx.at[1, rz, PLACE[2]], xrl.at[rz, 1], x_dev[-1])
            give_x(rz, 2, tx.at[1, rz, PLACE[1]], xin.at[rz, 0, 1], x_dev[1])
        else:
            give_x(rz, 3, tx.at[0, rz, PLACE[3]], xin.at[rz, 1, 0], x_dev[-1])

    def x_second(rz):
        for what, kind, rx, side, dev in ((0, 0, 1, 0, x_dev[1]), (1, 1, 3, 1, x_dev[-1])):
            at = PLACE[rx]
            sums[rz, what].wait_recv()
            tx[kind, rz, at] = (pf[kind, rz, at] + xrl[rz, kind].astype(F32)).astype(BF16)
            give_x(rz, 4 + kind, tx.at[kind, rz, at], xin.at[rz, side, kind], dev)

    def x_sum(rz):
        for what in (0, 1, 2, 3, 4, 5) if rz == 2 else (2, 3, 4, 5):
            sums[rz, what].wait_recv()
        for kind in range(2):
            both = xin[rz, 0, kind].astype(F32) + xin[rz, 1, kind].astype(F32)
            if rz == 2:
                both = both + xrl[rz, kind].astype(F32)
            xsum[rz, kind] = pf[kind, rz, own] + both

    def z_pass(what, src, dst, dev):
        sums[R, what] = remote(src, dst, z_send.at[what], z_recv.at[what], dev)
        late.append(sent.pop())

    def z_first(rz, what, kind, dst, dev):
        ztx[rz, kind] = xsum[rz, kind].astype(BF16)
        z_pass(what, ztx.at[rz, kind], dst, dev)

    def grad_step(rz, p):
        grad_pair(rz, p)
        x_first(rz, p)

    for rz in (2, 1, 3):
        grad_step(rz, 0)
        grad_step(rz, 1)
    grad_step(0, 0)
    x_second(1)
    grad_step(0, 1)
    x_sum(2)
    z_first(2, 0, 0, zrl.at[0], z_dev[1])
    z_first(2, 1, 1, zrl.at[1], z_dev[-1])
    x_second(3)
    x_second(0)
    x_sum(1)
    z_first(1, 2, 1, zin.at[0, 1], z_dev[1])
    x_sum(3)
    z_first(3, 3, 0, zin.at[1, 0], z_dev[-1])

    for c in range(HT // CH):
        part = slice(c * CH, (c + 1) * CH)
        grad_t = None
        for rz in range(R):
            for p in range(2):
                grads_2 = dsbuf[rz, pair_of(p), :, part].reshape(2 * T, CH)
                term = jnp.dot(kt[rz, p], grads_2, preferred_element_type=F32)
                grad_t = term if grad_t is None else grad_t + term
        for i in range(CH // T):
            h = c * (CH // T) + i
            dq_out[:, h * HD : (h + 1) * HD] = grad_t[:, i * T : (i + 1) * T].T.astype(BF16)
    dq_copy = pltpu.make_async_copy(dq_out, dq_hbm.at[0], out_sem.at[0])
    dq_copy.start()
    drain(sent)

    for what, kind, rz, side, dev in ((0, 0, 1, 0, z_dev[1]), (1, 1, 3, 1, z_dev[-1])):
        sums[R, what].wait_recv()
        ztx[rz, kind] = (xsum[rz, kind] + zrl[kind].astype(F32)).astype(BF16)
        z_pass(4 + kind, ztx.at[rz, kind], zin.at[side, kind], dev)
    x_sum(0)
    for what in (2, 3, 4, 5):
        sums[R, what].wait_recv()
    for kind, out in ((0, dk_ref), (1, dv_ref)):
        both = zin[0, kind].astype(F32) + zin[1, kind].astype(F32)
        out[0] = (xsum[0, kind] + both).astype(BF16)

    drain(late)
    dq_copy.wait()


def body(queries, keys, values, outputs, out_grad, positions, tile_flags):
    block = jax.ShapeDtypeStruct((1, T, HD), BF16)
    hbm = pl.BlockSpec(memory_space=pl.ANY)
    vmem = pl.BlockSpec(memory_space=pltpu.VMEM)
    dma = pltpu.SemaphoreType.DMA
    return pl.pallas_call(
        kernel,
        out_shape=(jax.ShapeDtypeStruct((1, T, H * HD), BF16), block, block),
        in_specs=[hbm] * 7,
        out_specs=(hbm, vmem, vmem),
        scratch_shapes=[
            pltpu.VMEM((T, H * HD), BF16),
            pltpu.VMEM((T, H * HD), BF16),
            pltpu.VMEM((T, H * HD), BF16),
            pltpu.VMEM((1, R * R * T), jnp.int32),
            pltpu.SMEM((1, 1, R * R), jnp.int32),
            pltpu.VMEM((HT, HD), BF16),
            pltpu.VMEM((HT, HD), BF16),
            pltpu.VMEM((HD, HT), BF16),
            pltpu.VMEM((HD, HT), BF16),
            pltpu.VMEM((2, R, R, T, HD), BF16),
            pltpu.VMEM((R, 2, HD, 2 * T), BF16),
            pltpu.VMEM((T, T), F32),
            pltpu.VMEM((R, R, T, T), F32),
            pltpu.VMEM((R, R, T, HT), F32),
            pltpu.VMEM((R, R, T, HT), BF16),
            pltpu.VMEM((8, HT), F32),
            pltpu.VMEM((8, HT), F32),
            pltpu.VMEM((1, HT), F32),
            pltpu.VMEM((1, HT), F32),
            pltpu.VMEM((2, R, R, T, HD), F32),
            pltpu.VMEM((2, R, R, T, HD), BF16),
            pltpu.VMEM((R, 2, T, HD), BF16),
            pltpu.VMEM((R, 2, 2, T, HD), BF16),
            pltpu.VMEM((R, 2, T, HD), F32),
            pltpu.VMEM((R, 2, T, HD), BF16),
            pltpu.VMEM((2, T, HD), BF16),
            pltpu.VMEM((2, 2, T, HD), BF16),
            pltpu.VMEM((T, H * HD), BF16),
            dma((7,)),
            dma((1,)),
            dma((2, 2, R, R)),
            dma((2, 2, R, R)),
            dma((R, 6)),
            dma((R, 6)),
            dma((6,)),
            dma((6,)),
        ],
        compiler_params=pltpu.CompilerParams(
            collective_id=0, has_side_effects=True, vmem_limit_bytes=56 * 1024 * 1024
        ),
        name="attention_backward",
    )(queries, keys, values, outputs, out_grad, positions, tile_flags)


def solution(mesh):
    sharded = P("col", "row", None)
    placed = (sharded,) * 5 + (P("col", None), sharded)
    return jax.shard_map(
        body, mesh=mesh, in_specs=placed, out_specs=(sharded,) * 3, check_vma=False
    )
```

```python
import math

import jax
import jax.numpy as jnp
from jax import lax
from jax.experimental import pallas as pl
from jax.experimental.pallas import tpu as pltpu
from jax.sharding import PartitionSpec as P

H = 8
HD = 128
T = 128
R = 4
HT = H * T
CH = 256
NEG = -1e30
SCALE = 1.0 / math.sqrt(HD)
LOG2E = math.log2(math.e)
F32 = jnp.float32
BF16 = jnp.bfloat16
RX = (2, 1, 3, 0)
PLACE = {rx: place for place, rx in enumerate(RX)}
HALF = T // 2


def kernel(
    q_hbm, k_hbm, v_hbm, o_hbm, g_hbm, pos_hbm, flag_hbm,
    dq_hbm, dk_ref, dv_ref,
    q_in, o_in, g_in, pos_ref, flag_ref, qs, gs, q_cols, g_cols, kv, kt, pos_rows, bias, sbuf, dsbuf,
    top, total, lse, dot_row, pf, tx, xrl, xin, xsum, ztx, zrl, zin, dq_out,
    in_sem, out_sem, gather_send, gather_recv, x_send, x_recv, z_send, z_recv,
):
    me = lax.axis_index("row")
    zh = me // R
    x = me % R
    z_dev = {1: ((zh + 1) % R) * R + x, -1: ((zh + R - 1) % R) * R + x}
    x_dev = {1: zh * R + (x + 1) % R, 2: zh * R + (x + 2) % R, -1: zh * R + (x + R - 1) % R}

    own = PLACE[0]
    k_copy = pltpu.make_async_copy(k_hbm.at[0], kv.at[0, 0, own], in_sem.at[0])
    v_copy = pltpu.make_async_copy(v_hbm.at[0], kv.at[1, 0, own], in_sem.at[1])
    g_copy = pltpu.make_async_copy(g_hbm.at[0], g_in, in_sem.at[2])
    o_copy = pltpu.make_async_copy(o_hbm.at[0], o_in, in_sem.at[3])
    q_copy = pltpu.make_async_copy(q_hbm.at[0], q_in, in_sem.at[4])
    pos_copy = pltpu.make_async_copy(pos_hbm, pos_ref, in_sem.at[5])
    flag_copy = pltpu.make_async_copy(flag_hbm, flag_ref, in_sem.at[6])
    for copy in (k_copy, v_copy, pos_copy, flag_copy, q_copy, g_copy, o_copy):
        copy.start()

    barrier = pltpu.get_barrier_semaphore()
    for dev in (z_dev[1], z_dev[-1], x_dev[1], x_dev[2], x_dev[-1]):
        pl.semaphore_signal(
            barrier, inc=1, device_id={"row": dev}, device_id_type=pl.DeviceIdType.MESH
        )

    sent = []

    def remote(src, dst, send, recv, dev):
        copy = pltpu.make_async_remote_copy(
            src_ref=src, dst_ref=dst, send_sem=send, recv_sem=recv,
            device_id={"row": dev}, device_id_type=pl.DeviceIdType.MESH,
        )
        copy.start()
        sent.append(copy)
        return copy

    late = []

    def drain(copies):
        while copies:
            copies.pop().wait_send()

    incoming = {}

    def give(kind, src, dst, dev, halves=(None,)):
        (rz, rx), (to_rz, to_rx) = src, dst
        at, to = PLACE[rx], PLACE[to_rx]
        for half in halves:
            rows = pl.ds(0, T) if half is None else pl.ds(half * HALF, HALF)
            incoming.setdefault((kind, dst), []).append(
                remote(
                    kv.at[kind, rz, at, rows, :], kv.at[kind, to_rz, to, rows, :],
                    gather_send.at[kind, half or 0, to_rz, to],
                    gather_recv.at[kind, half or 0, to_rz, to], dev,
                )
            )

    def got(kind, slot):
        for copy in incoming.pop((kind, slot), ()):
            copy.wait_recv()

    def along_z():
        give(0, (0, 0), (3, 0), z_dev[1], (0, 1))
        give(1, (0, 0), (1, 0), z_dev[-1], (0, 1))
        give(1, (0, 0), (3, 0), z_dev[1])
        give(0, (0, 0), (1, 0), z_dev[-1])

    def onward_z():
        for half in range(2):
            for kind, slot, dev in ((0, (3, 0), z_dev[1]), (1, (1, 0), z_dev[-1])):
                incoming[kind, slot].pop(0).wait_recv()
                give(kind, slot, (2, 0), dev, (half,))

    def along_x(rz):
        give(0, (rz, 0), (rz, 3), x_dev[1])
        give(1, (rz, 0), (rz, 1), x_dev[-1])
        give(1, (rz, 0), (rz, 3), x_dev[1])
        give(0, (rz, 0), (rz, 1), x_dev[-1])

    def onward_x(rz):
        for kind in range(2):
            slot = (rz, 1 if kind else 3)
            got(kind, slot)
            give(kind, slot, (rz, 2), x_dev[-1 if kind else 1])

    def all_of(kind, rz):
        for rx in range(R):
            got(kind, (rz, rx))

    def block_of(rz, place):
        return ((zh + rz) % R) * R + (x + RX[place]) % R

    slots = [(rz, place) for rz in range(R) for place in range(R)]
    k_copy.wait()
    v_copy.wait()
    pl.semaphore_wait(barrier, 5)

    along_z()
    along_x(0)

    pos_copy.wait()
    flag_copy.wait()
    pos_rows[...] = jnp.zeros_like(pos_rows)
    for i, slot in enumerate(slots):
        row = pos_ref[:, pl.ds(pl.multiple_of(block_of(*slot) * T, T), T)]
        pos_rows[i : i + 1, :] = row.astype(F32)
    pos_cols = pos_rows[...].T
    for i, (rz, place) in enumerate(slots):
        own_pos = pos_rows[own : own + 1, :]
        off = (flag_ref[0, 0, block_of(rz, place)] - 1).astype(F32) * (-NEG)
        column = jnp.broadcast_to(pos_cols[:, i : i + 1], (T, T))
        value = jnp.where(column <= own_pos, 0.0, NEG) + off
        if (rz, place) == (0, own):
            keys_at = lax.broadcasted_iota(jnp.int32, (T, T), 0)
            queries_at = lax.broadcasted_iota(jnp.int32, (T, T), 1)
            value = jnp.where(keys_at == queries_at, 0.0, value)
        bias[rz, place] = value

    q_copy.wait()
    for h in range(H):
        head = q_in[:, h * HD : (h + 1) * HD]
        qs[h * T : (h + 1) * T, :] = head
        q_cols[:, h * T : (h + 1) * T] = head.T
    g_copy.wait()
    o_copy.wait()
    for h in range(H):
        cols = slice(h * HD, (h + 1) * HD)
        head = g_in[:, cols]
        gs[h * T : (h + 1) * T, :] = head
        g_cols[:, h * T : (h + 1) * T] = head.T
        product = head.astype(F32) * o_in[:, cols].astype(F32)
        dot_row[:, h * T : (h + 1) * T] = jnp.sum(product.T, axis=0, keepdims=True)

    top[...] = jnp.full_like(top, NEG)
    total[...] = jnp.zeros_like(total)

    def pair_of(p):
        return pl.ds(2 * p, 2)

    def score_pair(rz, p):
        pair = pair_of(p)
        keys_2 = kv[0, rz, pair].reshape(2 * T, HD)
        kt[rz, p] = keys_2.T
        mask = bias[rz, pair].reshape(2 * T, T)
        mask = jnp.concatenate([mask] * (CH // T), axis=1)
        for c in range(HT // CH):
            part = slice(c * CH, (c + 1) * CH)
            raw = jnp.dot(keys_2, q_cols[:, part], preferred_element_type=F32)
            score = raw * (SCALE * LOG2E) + mask
            sbuf[rz, pair, :, part] = score.reshape(2, T, CH)
            parts = score.reshape(2 * T // 8, 8, CH)
            old = top[:, part]
            new = jnp.maximum(old, jnp.max(parts, axis=0))
            added = jnp.sum(jnp.exp2(parts - new[None]), axis=0)
            total[:, part] = total[:, part] * jnp.exp2(old - new) + added
            top[:, part] = new

    def score_group(rz):
        def step(p, carry):
            score_pair(rz, p)
            return carry

        lax.fori_loop(0, 2, step, 0)

    onward_x(0)
    onward_z()
    got(1, (3, 0))
    along_x(3)
    got(0, (1, 0))
    along_x(1)
    all_of(0, 0)
    score_group(0)
    onward_x(3)
    onward_x(1)
    all_of(0, 3)
    score_group(3)
    got(0, (2, 0))
    give(0, (2, 0), (2, 2), x_dev[2])
    give(0, (2, 0), (2, 3), x_dev[1])
    give(0, (2, 0), (2, 1), x_dev[-1])
    got(1, (2, 0))
    give(1, (2, 0), (2, 2), x_dev[2])
    give(1, (2, 0), (2, 1), x_dev[-1])
    give(1, (2, 0), (2, 3), x_dev[1])
    all_of(0, 1)
    score_group(1)
    got(0, (2, 3))
    score_pair(2, 1)
    all_of(0, 2)
    score_pair(2, 0)

    top_all = jnp.max(top[...], axis=0, keepdims=True)
    total_all = jnp.sum(total[...] * jnp.exp2(top[...] - top_all), axis=0, keepdims=True)
    lse[...] = top_all + jnp.log(total_all) * LOG2E
    for rz in (2, 1, 3, 0):
        all_of(1, rz)

    def grad_pair(rz, p):
        pair = pair_of(p)
        values_2 = kv[1, rz, pair].reshape(2 * T, HD)
        dk = dv = None
        for c in range(HT // CH):
            part = slice(c * CH, (c + 1) * CH)
            probs = jnp.dot(values_2, g_cols[:, part], preferred_element_type=F32)
            weights = jnp.exp2(sbuf[rz, pair, :, part].reshape(2 * T, CH) - lse[:, part])
            grads = (weights * (probs - dot_row[:, part]) * SCALE).astype(BF16)
            dsbuf[rz, pair, :, part] = grads.reshape(2, T, CH)
            dk_c = jnp.dot(grads, qs[part, :], preferred_element_type=F32)
            dv_c = jnp.dot(weights.astype(BF16), gs[part, :], preferred_element_type=F32)
            dk = dk_c if c == 0 else dk + dk_c
            dv = dv_c if c == 0 else dv + dv_c
        for kind, grad in ((0, dk), (1, dv)):
            grad = grad.reshape(2, T, HD)
            pf[kind, rz, pair] = grad
            tx[kind, rz, pair] = grad.astype(BF16)

    sums = {}

    def give_x(rz, what, src, dst, dev):
        sums[rz, what] = remote(src, dst, x_send.at[rz, what], x_recv.at[rz, what], dev)

    def x_first(rz, p):
        if rz == 2 and p == 0:
            for kind in range(2):
                give_x(rz, kind, tx.at[kind, rz, PLACE[2]], xrl.at[rz, kind], x_dev[2])
            for kind, what in ((0, 4), (1, 2)):
                give_x(rz, what, tx.at[kind, rz, PLACE[1]], xin.at[rz, 0, kind], x_dev[1])
        elif rz == 2:
            for kind, what in ((0, 3), (1, 5)):
                give_x(rz, what, tx.at[kind, rz, PLACE[3]], xin.at[rz, 1, kind], x_dev[-1])
        elif p == 0:
            give_x(rz, 0, tx.at[0, rz, PLACE[2]], xrl.at[rz, 0], x_dev[1])
            give_x(rz, 1, tx.at[1, rz, PLACE[2]], xrl.at[rz, 1], x_dev[-1])
            give_x(rz, 2, tx.at[1, rz, PLACE[1]], xin.at[rz, 0, 1], x_dev[1])
        else:
            give_x(rz, 3, tx.at[0, rz, PLACE[3]], xin.at[rz, 1, 0], x_dev[-1])

    def x_second(rz):
        for what, kind, rx, side, dev in ((0, 0, 1, 0, x_dev[1]), (1, 1, 3, 1, x_dev[-1])):
            at = PLACE[rx]
            sums[rz, what].wait_recv()
            tx[kind, rz, at] = (pf[kind, rz, at] + xrl[rz, kind].astype(F32)).astype(BF16)
            give_x(rz, 4 + kind, tx.at[kind, rz, at], xin.at[rz, side, kind], dev)

    def x_sum(rz):
        for what in (0, 1, 2, 3, 4, 5) if rz == 2 else (2, 3, 4, 5):
            sums[rz, what].wait_recv()
        for kind in range(2):
            both = xin[rz, 0, kind].astype(F32) + xin[rz, 1, kind].astype(F32)
            if rz == 2:
                both = both + xrl[rz, kind].astype(F32)
            xsum[rz, kind] = pf[kind, rz, own] + both

    def z_pass(what, src, dst, dev):
        sums[R, what] = remote(src, dst, z_send.at[what], z_recv.at[what], dev)
        late.append(sent.pop())

    def z_first(rz, what, kind, dst, dev):
        ztx[rz, kind] = xsum[rz, kind].astype(BF16)
        z_pass(what, ztx.at[rz, kind], dst, dev)

    def grad_step(rz, p):
        grad_pair(rz, p)
        x_first(rz, p)

    for rz in (2, 1, 3):
        grad_step(rz, 0)
        grad_step(rz, 1)
    grad_step(0, 0)
    x_second(1)
    grad_step(0, 1)
    x_sum(2)
    z_first(2, 0, 0, zrl.at[0], z_dev[1])
    z_first(2, 1, 1, zrl.at[1], z_dev[-1])
    x_second(3)
    x_second(0)
    x_sum(1)
    z_first(1, 2, 1, zin.at[0, 1], z_dev[1])
    x_sum(3)
    z_first(3, 3, 0, zin.at[1, 0], z_dev[-1])

    for c in range(HT // CH):
        part = slice(c * CH, (c + 1) * CH)
        grad_t = None
        for rz in range(R):
            for p in range(2):
                grads_2 = dsbuf[rz, pair_of(p), :, part].reshape(2 * T, CH)
                term = jnp.dot(kt[rz, p], grads_2, preferred_element_type=F32)
                grad_t = term if grad_t is None else grad_t + term
        for i in range(CH // T):
            h = c * (CH // T) + i
            dq_out[:, h * HD : (h + 1) * HD] = grad_t[:, i * T : (i + 1) * T].T.astype(BF16)
    dq_copy = pltpu.make_async_copy(dq_out, dq_hbm.at[0], out_sem.at[0])
    dq_copy.start()
    drain(sent)

    for what, kind, rz, side, dev in ((0, 0, 1, 0, z_dev[1]), (1, 1, 3, 1, z_dev[-1])):
        sums[R, what].wait_recv()
        ztx[rz, kind] = (xsum[rz, kind] + zrl[kind].astype(F32)).astype(BF16)
        z_pass(4 + kind, ztx.at[rz, kind], zin.at[side, kind], dev)
    x_sum(0)
    for what in (2, 3, 4, 5):
        sums[R, what].wait_recv()
    for kind, out in ((0, dk_ref), (1, dv_ref)):
        both = zin[0, kind].astype(F32) + zin[1, kind].astype(F32)
        out[0] = (xsum[0, kind] + both).astype(BF16)

    drain(late)
    dq_copy.wait()


def body(queries, keys, values, outputs, out_grad, positions, tile_flags):
    block = jax.ShapeDtypeStruct((1, T, HD), BF16)
    hbm = pl.BlockSpec(memory_space=pl.ANY)
    vmem = pl.BlockSpec(memory_space=pltpu.VMEM)
    dma = pltpu.SemaphoreType.DMA
    return pl.pallas_call(
        kernel,
        out_shape=(jax.ShapeDtypeStruct((1, T, H * HD), BF16), block, block),
        in_specs=[hbm] * 7,
        out_specs=(hbm, vmem, vmem),
        scratch_shapes=[
            pltpu.VMEM((T, H * HD), BF16),
            pltpu.VMEM((T, H * HD), BF16),
            pltpu.VMEM((T, H * HD), BF16),
            pltpu.VMEM((1, R * R * T), jnp.int32),
            pltpu.SMEM((1, 1, R * R), jnp.int32),
            pltpu.VMEM((HT, HD), BF16),
            pltpu.VMEM((HT, HD), BF16),
            pltpu.VMEM((HD, HT), BF16),
            pltpu.VMEM((HD, HT), BF16),
            pltpu.VMEM((2, R, R, T, HD), BF16),
            pltpu.VMEM((R, 2, HD, 2 * T), BF16),
            pltpu.VMEM((T, T), F32),
            pltpu.VMEM((R, R, T, T), F32),
            pltpu.VMEM((R, R, T, HT), F32),
            pltpu.VMEM((R, R, T, HT), BF16),
            pltpu.VMEM((8, HT), F32),
            pltpu.VMEM((8, HT), F32),
            pltpu.VMEM((1, HT), F32),
            pltpu.VMEM((1, HT), F32),
            pltpu.VMEM((2, R, R, T, HD), F32),
            pltpu.VMEM((2, R, R, T, HD), BF16),
            pltpu.VMEM((R, 2, T, HD), BF16),
            pltpu.VMEM((R, 2, 2, T, HD), BF16),
            pltpu.VMEM((R, 2, T, HD), F32),
            pltpu.VMEM((R, 2, T, HD), BF16),
            pltpu.VMEM((2, T, HD), BF16),
            pltpu.VMEM((2, 2, T, HD), BF16),
            pltpu.VMEM((T, H * HD), BF16),
            dma((7,)),
            dma((1,)),
            dma((2, 2, R, R)),
            dma((2, 2, R, R)),
            dma((R, 6)),
            dma((R, 6)),
            dma((6,)),
            dma((6,)),
        ],
        compiler_params=pltpu.CompilerParams(
            collective_id=0, has_side_effects=True, vmem_limit_bytes=56 * 1024 * 1024
        ),
        name="attention_backward",
    )(queries, keys, values, outputs, out_grad, positions, tile_flags)


def solution(mesh):
    sharded = P("col", "row", None)
    placed = (sharded,) * 5 + (P("col", None), sharded)
    return jax.shard_map(
        body, mesh=mesh, in_specs=placed, out_specs=(sharded,) * 3, check_vma=False
    )
```
